32 devices in a mesh: param: 16 (over z, y, x), sensor: 2 (over core).
Axes of the slice: x: 2, y: 2, z: 4, core: 2. Of those that a mesh axis runs over, the one named last changes fastest.
Arguments:
- data: float32 [16, 512, 420], P(None, ('sensor', 'param')), may hold values from -6 to 6
- spectra: float32 [2, 512, 64, 421], P(None, 'sensor', 'param'), may hold values from -2 to 2
Outputs:
- gradient: float32 [16, 64, 420], P(None, 'param')
- rms: float32 [16], replicated
The draws below stay inside these ranges and needn't reach their ends.
All inputs are finite; a program needn't handle non-finite values.
Results may differ from the reference program's by a relative error of at most 0.0003.
Values sent between devices are 32-bit elements; how exact they have to be, the bound alone decides.
A program may use at most 128 MiB of HBM per device.

```python
import math
import jax
import jax.numpy as jnp
from jax import lax

SENSORS = 512
NT = 420
NF = 421
P_DEV = 4
NRHS = 16
PARAMS = 64
N_PARAM = 16


def draw_spectra(key, part):
    first = jax.random.fold_in(key, 0)
    shape = (2, SENSORS, PARAMS, NF)
    ramp = 1.0 + jnp.arange(PARAMS, dtype=jnp.float32) / max(PARAMS - 1, 1)
    base = jnp.clip(jax.random.normal(first, shape, jnp.float32), -6.0, 6.0)
    base = base * ramp[None, None, :, None]
    return jnp.clip(base / math.sqrt(SENSORS), -2.0, 2.0)


def shard_levels(rng, dims, cuts, smallest, largest):
    gain = 1.0
    for dim, blocks in cuts:
        heights = jax.random.uniform(jax.random.fold_in(jax.random.fold_in(rng, 6), dim), (blocks,), jnp.float32, smallest / len(cuts), largest / len(cuts))
        gain = gain * jnp.repeat(jnp.exp(heights), dims[dim] // blocks).reshape((-1,) + (1,) * (len(dims) - 1 - dim))
    return gain


def gaussian(rng, shape, scale, limit, shards=(), kind=jnp.bfloat16):
    values = jax.random.normal(rng, shape, jnp.float32) * scale
    if len(shards) > 0:
        values = shard_levels(rng, shape, shards, -0.22, 0.18) * values
    return jnp.clip(values, min=-limit, max=limit).astype(kind)


def setup_inputs(seed: int = 0) -> dict:
    seeds = jax.random.split(jax.random.key(seed), 3)
    data = gaussian(seeds[0], (NRHS, SENSORS, NT), 1.0, 6.0, ((1, 32),), jnp.float32)
    spectra = draw_spectra(jax.random.fold_in(seeds[2], 71), 0)
    return dict(data=data, spectra=spectra)


def reference(data, spectra):
    data_hat = jnp.fft.rfft(data, n=2 * NT, axis=-1)
    real_part = jnp.real(data_hat).astype(jnp.float32)
    imag_part = jnp.imag(data_hat).astype(jnp.float32)

    def one_block(index):
        start = (index * P_DEV).astype(jnp.int32)
        kernel = lax.dynamic_slice_in_dim(spectra, start, P_DEV, 2)
        kernel_re = kernel[0]
        kernel_im = kernel[1]
        hi = lax.Precision.HIGHEST
        out_re = jnp.einsum('spf,rsf->rpf', kernel_re, real_part, precision=hi) + jnp.einsum('spf,rsf->rpf', kernel_im, imag_part, precision=hi)
        out_im = jnp.einsum('spf,rsf->rpf', kernel_re, imag_part, precision=hi) - jnp.einsum('spf,rsf->rpf', kernel_im, real_part, precision=hi)
        return (out_re, out_im)
    blocks_re, blocks_im = lax.map(one_block, jnp.arange(N_PARAM, dtype=jnp.int32))
    whole_re = jnp.transpose(blocks_re, (1, 0, 2, 3)).reshape(data.shape[0], PARAMS, NF)
    whole_im = jnp.transpose(blocks_im, (1, 0, 2, 3)).reshape(data.shape[0], PARAMS, NF)
    field = jnp.fft.irfft(whole_re + 1j * whole_im, n=2 * NT, axis=-1)[..., :NT].astype(jnp.float32)
    rms = jnp.sqrt(lax.optimization_barrier(jnp.mean(field * field, axis=(1, 2))) + 1e-06)
    return (field / rms[:, None, None], rms)
```

```python
import functools
import math

import jax
import jax.numpy as jnp
import numpy as np
from jax import lax
from jax.experimental import pallas as pl
from jax.experimental.pallas import tpu as pltpu
from jax.sharding import PartitionSpec as P

MESH = pl.DeviceIdType.MESH
LANES = 128
GROUP = 8
CHUNKS = 4


def spectral_tables(steps):
    length = 2 * steps
    freqs = steps + 1
    times = lax.broadcasted_iota(jnp.int32, (steps, freqs), 0)
    bins = lax.broadcasted_iota(jnp.int32, (steps, freqs), 1)
    phase = 2.0 * math.pi / length * (times * bins % length).astype(jnp.float32)
    forward = jnp.concatenate([jnp.cos(phase), -jnp.sin(phase)], axis=1)
    weight = jnp.where((bins == 0) | (bins == steps), 1.0, 2.0) / length
    backward = jnp.concatenate([(weight * jnp.cos(phase)).T, (-weight * jnp.sin(phase)).T], axis=0)
    return (forward, backward)


def to_spectrum(series, forward):
    vectors, sensors, steps = series.shape
    flat = jnp.dot(
        series.reshape(vectors * sensors, steps),
        forward,
        precision=lax.Precision.HIGHEST,
        preferred_element_type=jnp.float32,
    )
    return flat.reshape(vectors, sensors, forward.shape[1])


def contract(kernel, spectrum):
    return jnp.einsum(
        "spf,rsf->rpf",
        kernel,
        spectrum,
        precision=lax.Precision.HIGHEST,
        preferred_element_type=jnp.float32,
    )


def general_body(data, spectra):
    steps = data.shape[2]
    freqs = steps + 1
    forward, backward = spectral_tables(steps)
    whole = to_spectrum(lax.all_gather(data, "param", axis=1, tiled=True), forward)
    real_part = whole[..., :freqs]
    imag_part = whole[..., freqs:]
    kernel_re = spectra[0]
    kernel_im = spectra[1]
    out_re = contract(kernel_re, real_part) + contract(kernel_im, imag_part)
    out_im = contract(kernel_re, imag_part) - contract(kernel_im, real_part)
    vectors, points = (out_re.shape[0], out_re.shape[1])
    stacked = jnp.concatenate([out_re, out_im], axis=2).reshape(vectors * points, 2 * freqs)
    partial_field = jnp.dot(
        stacked, backward, precision=lax.Precision.HIGHEST, preferred_element_type=jnp.float32
    ).reshape(vectors, points, steps)
    count = points * lax.axis_size("param") * steps
    share = lax.psum_scatter(partial_field, "sensor", scatter_dimension=0, tiled=True)
    squares = lax.psum(jnp.sum(share * share, axis=(1, 2)), "param")
    scale = jnp.sqrt(squares / count + 1e-06)
    normalized = share / scale[:, None, None]
    gradient, rms_all = (
        lax.all_gather(normalized, "sensor", axis=0, tiled=True),
        lax.all_gather(scale, "sensor", axis=0, tiled=True),
    )
    return (gradient, rms_all)


def split(value):
    high = value.astype(jnp.bfloat16)
    return high, (value - high.astype(jnp.float32)).astype(jnp.bfloat16)


NT_DIMS = (((1,), (1,)), ((), ()))


def product(left, right, dims):
    dot = functools.partial(lax.dot_general, dimension_numbers=dims, preferred_element_type=jnp.float32)
    return dot(left[0], right[0]) + (dot(left[0], right[1]) + dot(left[1], right[0]))


def kernel(
    n, lines, vectors, local, steps, points, freqs, padded, wide,
    data_ref, spectra_ref, table_ref,
    out_ref, rms_ref,
    gathered, kbuf, table, even_h, even_l, odd_h, odd_l, spectrum, product_s, partial, pairs, square, squares,
    load_sem, swap_send, swap_recv, kswap_send, kswap_recv, z_send, z_recv, y_send, y_recv, c_send, c_recv,
    f_send, f_recv, r_send, r_recv,
):
    me = lax.axis_index("param")
    core = lax.axis_index("sensor")
    x = lax.rem(me, 2)
    y = lax.rem(me // 2, 2)
    z = me // 4
    plane = 4
    other_chip = me + 1 - 2 * x
    y_chip = me + 2 - 4 * y
    other_core = 1 - core
    swapped = x != core
    kept = x == core
    per = (vectors // 2) // CHUNKS

    table_copy = pltpu.make_async_copy(table_ref, table, load_sem.at[0])
    table_copy.start()
    kbuf[:, freqs:] = jnp.zeros((2, padded - freqs) + tuple(kbuf.shape[2:]), jnp.float32)

    barrier = pltpu.get_barrier_semaphore()

    @pl.loop(1, n)
    def _(step):
        pl.semaphore_signal(barrier, inc=1, device_id=(lax.rem(me + step, n), core), device_id_type=MESH)

    pl.semaphore_signal(barrier, inc=1, device_id=(me, other_core), device_id_type=MESH)
    pl.semaphore_signal(barrier, inc=1, device_id=(other_chip, other_core), device_id_type=MESH)
    pl.semaphore_wait(barrier, n + 1)

    def slot(line, row, column):
        return line * plane + row * 2 + column

    def block(chunk, position):
        return gathered.at[pl.ds(chunk * per, per), pl.ds(pl.multiple_of(position * local, local), local), :]

    mine = slot(z, y, core)

    def swap(chunk):
        return pltpu.make_async_remote_copy(
            src_ref=data_ref.at[pl.ds(chunk * per, per)],
            dst_ref=block(chunk, slot(z, y, other_core)),
            send_sem=swap_send.at[chunk], recv_sem=swap_recv.at[chunk],
            device_id=(other_chip, other_core), device_id_type=MESH,
        )

    def keep(chunk):
        return pltpu.make_async_copy(data_ref.at[pl.ds(chunk * per, per)], block(chunk, mine), swap_recv.at[chunk])

    def kswap(part):
        return pltpu.make_async_remote_copy(
            src_ref=spectra_ref.at[part], dst_ref=kbuf.at[part, pl.ds(0, freqs)],
            send_sem=kswap_send.at[part], recv_sem=kswap_recv.at[part],
            device_id=(other_chip, other_core), device_id_type=MESH,
        )

    def kkeep(part):
        return pltpu.make_async_copy(spectra_ref.at[part], kbuf.at[part, pl.ds(0, freqs)], kswap_recv.at[part])

    @pl.when(swapped)
    def _():
        for chunk in range(CHUNKS):
            swap(chunk).start()
        for part in range(2):
            kswap(part).start()

    @pl.when(kept)
    def _():
        for chunk in range(CHUNKS):
            keep(chunk).start()
        for part in range(2):
            kkeep(part).start()

    def send(chunk, position, target, send_sem, recv_sem):
        return pltpu.make_async_remote_copy(
            src_ref=block(chunk, position), dst_ref=block(chunk, position),
            send_sem=send_sem, recv_sem=recv_sem, device_id=target, device_id_type=MESH,
        )

    def line_copy(chunk, step):
        target = lax.rem(z + step, lines)
        return send(chunk, mine, (slot(target, y, x), core), z_send.at[chunk, step], z_recv.at[chunk, step])

    def y_copy(chunk, step):
        return send(
            chunk, slot(lax.rem(z + lines - step, lines), y, core), (y_chip, core),
            y_send.at[chunk, step], y_recv.at[chunk, step],
        )

    def core_copy(chunk, row, step):
        position = slot(lax.rem(z + lines - step, lines), row, core)
        index = step + lines * jnp.where(row == y, 0, 1)
        return send(chunk, position, (me, other_core), c_send.at[chunk, index], c_recv.at[chunk, index])

    def start_lines(chunk):
        @pl.when(swapped)
        def _():
            swap(chunk).wait_recv()

        @pl.when(kept)
        def _():
            keep(chunk).wait()

        for step in range(1, lines):
            line_copy(chunk, step).start()
        y_copy(chunk, 0).start()
        core_copy(chunk, y, 0).start()

    def from_lines(chunk):
        for step in range(1, lines):
            line_copy(chunk, step).wait_recv()
            y_copy(chunk, step).start()
            core_copy(chunk, y, step).start()

    def from_row(chunk):
        for step in range(lines):
            y_copy(chunk, step).wait_recv()
            core_copy(chunk, 1 - y, step).start()

    def from_core(chunk):
        for step in range(lines):
            core_copy(chunk, y, step).wait_recv()
            core_copy(chunk, 1 - y, step).wait_recv()

    def transform(chunk):
        @pl.loop(0, per)
        def _(pair):
            r2 = chunk * per + pair
            for half, high, low in ((0, even_h, even_l), (1, odd_h, odd_l)):
                begin = half * (gathered.shape[2] - wide)
                series = split(gathered[r2, :, begin : begin + wide])

                @pl.loop(0, 2)
                def _(imag):
                    rows = pl.ds(pl.multiple_of(imag * padded, 16), padded)
                    result = product((high[rows, :], low[rows, :]), series, NT_DIMS)
                    for lane in range(2):
                        spectrum[lane, pl.ds(imag * vectors + 2 * r2 + half, padded, stride=2 * vectors), :] = result[
                            :, lane * LANES : (lane + 1) * LANES
                        ]

    for chunk in range(CHUNKS):
        start_lines(chunk)

    table_copy.wait()
    shift = 2 * steps - (gathered.shape[2] - wide) - steps
    values = table[...]
    even_h[...], even_l[...] = split(values)
    odd_h[...], odd_l[...] = split(pltpu.roll(values, shift, 1))

    from_lines(0)
    for chunk in range(CHUNKS):
        if chunk + 1 < CHUNKS:
            from_lines(chunk + 1)
        from_row(chunk)
        from_core(chunk)
        transform(chunk)

    @pl.when(swapped)
    def _():
        for part in range(2):
            kswap(part).wait_recv()

    @pl.when(kept)
    def _():
        for part in range(2):
            kkeep(part).wait()

    rows = GROUP * points
    columns = GROUP * 2 * vectors
    row_freq = lax.broadcasted_iota(jnp.int32, (2 * rows, columns), 0) // points % GROUP
    col_freq = lax.broadcasted_iota(jnp.int32, (2 * rows, columns), 1) // (2 * vectors)
    own = row_freq == col_freq
    lane = lax.broadcasted_iota(jnp.int32, (rows, LANES), 1)
    sign = jnp.where(lane % (2 * vectors) < vectors, 1.0, -1.0)
    row = lax.broadcasted_iota(jnp.int32, (rows, LANES), 0) // points

    @pl.loop(0, padded // GROUP)
    def _(group):
        begin = pl.multiple_of(group * columns, columns)
        right = split(
            jnp.concatenate([spectrum[0, pl.ds(begin, columns), :], spectrum[1, pl.ds(begin, columns), :]], axis=1)
        )
        left = jnp.concatenate(
            [kbuf[part, pl.ds(group * GROUP, GROUP)].reshape(rows, kbuf.shape[3]) for part in range(2)], axis=0
        )
        found = jnp.where(own, product(split(left), right, NT_DIMS), 0.0)
        width = columns
        while width > LANES:
            width //= 2
            found = found[:, :width] + found[:, width:]
        hop = LANES // 2
        while hop >= 2 * vectors:
            found = found + pltpu.roll(found, hop, 1)
            hop //= 2
        value = found[:rows] + sign * pltpu.roll(found[rows:], vectors, 1)
        freq = row + group * GROUP
        weight = jnp.where((freq == 0) | (freq == freqs - 1), 0.5 / steps, 1.0 / steps)
        product_s[pl.ds(pl.multiple_of(group * rows, rows), rows), :] = value * weight

    lanes = lax.broadcasted_iota(jnp.int32, (padded, LANES), 1) // (2 * vectors)
    merged = jnp.zeros((padded, LANES), jnp.float32)
    for point in range(points):
        merged = jnp.where(lanes == point, product_s[pl.ds(point, padded, stride=points), :], merged)
    turned = split(merged.T)
    plain = (((1,), (0,)), ((), ()))
    real = product(turned, (even_h[:padded, :], even_l[:padded, :]), plain)
    imag = product(turned, (even_h[padded:, :], even_l[padded:, :]), plain)
    for point in range(points):
        first = point * 2 * vectors
        field = real[first : first + vectors] + imag[first + vectors : first + 2 * vectors]
        partial[point * vectors : (point + 1) * vectors, :] = field

    def field_copy(target):
        return pltpu.make_async_remote_copy(
            src_ref=partial, dst_ref=pairs.at[x], send_sem=f_send.at[target], recv_sem=f_recv.at[x],
            device_id=(me - x + core, target), device_id_type=MESH,
        )

    def field_arrival(group):
        return pltpu.make_async_remote_copy(
            src_ref=partial, dst_ref=pairs.at[group], send_sem=f_send.at[0], recv_sem=f_recv.at[group],
            device_id=(other_chip, other_core), device_id_type=MESH,
        )

    @pl.when(swapped)
    def _():
        field_copy(0).start()
        field_copy(1).start()

    @pl.when(kept)
    def _():
        field_copy(other_core).start()
        pairs[x] = partial[...]

    field_arrival(1 - x).wait_recv()

    @pl.when(swapped)
    def _():
        field_arrival(x).wait_recv()

    total = pairs[0] + pairs[1]
    energy = total * total
    folded = energy[:vectors]
    for point in range(1, points):
        folded = folded + energy[point * vectors : (point + 1) * vectors]
    summed = jnp.broadcast_to(jnp.sum(folded, axis=1, keepdims=True), (vectors, LANES))
    square[...] = summed
    squares[me] = summed

    def square_copy(step):
        return pltpu.make_async_remote_copy(
            src_ref=square, dst_ref=squares.at[me], send_sem=r_send.at[step], recv_sem=r_recv.at[step],
            device_id=(lax.rem(me + step, n), core), device_id_type=MESH,
        )

    def square_arrival(step):
        return pltpu.make_async_remote_copy(
            src_ref=square, dst_ref=squares.at[lax.rem(me + n - step, n)],
            send_sem=r_send.at[step], recv_sem=r_recv.at[step],
            device_id=(lax.rem(me + step, n), core), device_id_type=MESH,
        )

    @pl.loop(1, n)
    def _(step):
        square_copy(step).start()

    for chunk in range(CHUNKS):
        for step in range(1, lines):
            line_copy(chunk, step).wait_send()
        for step in range(lines):
            y_copy(chunk, step).wait_send()
            core_copy(chunk, y, step).wait_send()
            core_copy(chunk, 1 - y, step).wait_send()

    @pl.when(swapped)
    def _():
        for chunk in range(CHUNKS):
            swap(chunk).wait_send()
        for part in range(2):
            kswap(part).wait_send()
        field_copy(0).wait_send()
        field_copy(1).wait_send()

    @pl.when(kept)
    def _():
        field_copy(other_core).wait_send()

    @pl.loop(1, n)
    def _(step):
        square_arrival(step).wait()

    energy_all = squares[0]
    for device in range(1, n):
        energy_all = energy_all + squares[device]
    scale = jnp.sqrt(energy_all / (points * n * steps) + 1e-06)
    rms_ref[...] = scale
    inverse = scale[:, :1]
    for point in range(points):
        out_ref[point] = total[point * vectors : (point + 1) * vectors, :steps] / inverse


def paired_body(data, spectra):
    n = lax.axis_size("param")
    vectors, local, steps = data.shape
    sensors, points, freqs = spectra.shape[1:]
    wide = -(-steps // LANES) * LANES
    packed = -(-2 * steps // LANES) * LANES
    padded = -(-freqs // 16) * 16
    times = np.arange(steps)[None, :]
    bins = np.arange(freqs)[:, None]
    phase = np.pi / steps * (times * bins % (2 * steps))
    host = np.zeros((2, padded, wide), np.float32)
    host[0, :freqs, :steps] = np.cos(phase)
    host[1, :freqs, :steps] = -np.sin(phase)
    table = jnp.asarray(host.reshape(2 * padded, wide))
    lines = n // 4

    halves = data.reshape(vectors // 2, 2, local, steps)
    series = jnp.concatenate([halves[:, 0], halves[:, 1]], axis=-1)
    series = jnp.pad(series, ((0, 0), (0, 0), (0, packed - 2 * steps)))
    turned = jnp.transpose(spectra, (0, 3, 2, 1))

    hbm = pl.BlockSpec(memory_space=pl.ANY)
    vmem = pl.BlockSpec(memory_space=pltpu.VMEM)
    dma = pltpu.SemaphoreType.DMA
    f32, bf16 = jnp.float32, jnp.bfloat16
    fields, scale = pl.pallas_call(
        functools.partial(kernel, n, lines, vectors, local, steps, points, freqs, padded, wide),
        out_shape=(
            jax.ShapeDtypeStruct((points, vectors, steps), f32),
            jax.ShapeDtypeStruct((vectors, LANES), f32),
        ),
        in_specs=[hbm, hbm, hbm],
        out_specs=(vmem, vmem),
        scratch_shapes=[
            pltpu.VMEM((vectors // 2, sensors, packed), f32),
            pltpu.VMEM((2, padded, points, sensors), f32),
            pltpu.VMEM((2 * padded, wide), f32),
            pltpu.VMEM((2 * padded, wide), bf16),
            pltpu.VMEM((2 * padded, wide), bf16),
            pltpu.VMEM((2 * padded, wide), bf16),
            pltpu.VMEM((2 * padded, wide), bf16),
            pltpu.VMEM((2, padded * 2 * vectors, LANES), f32),
            pltpu.VMEM((padded * points, LANES), f32),
            pltpu.VMEM((points * vectors, wide), f32),
            pltpu.VMEM((2, points * vectors, wide), f32),
            pltpu.VMEM((vectors, LANES), f32),
            pltpu.VMEM((n, vectors, LANES), f32),
            dma((1,)),
            dma((CHUNKS,)), dma((CHUNKS,)),
            dma((2,)), dma((2,)),
            dma((CHUNKS, lines)), dma((CHUNKS, lines)),
            dma((CHUNKS, lines)), dma((CHUNKS, lines)),
            dma((CHUNKS, 2 * lines)), dma((CHUNKS, 2 * lines)),
            dma((2,)), dma((2,)),
            dma((n,)), dma((n,)),
        ],
        compiler_params=pltpu.CompilerParams(
            collective_id=0, has_side_effects=True, vmem_limit_bytes=60 * 1024 * 1024
        ),
    )(series, turned, table)
    return (jnp.transpose(fields, (1, 0, 2)), scale[:, 0])


def solution(mesh):
    in_specs = (P(None, ("sensor", "param"), None), P(None, "sensor", "param", None))
    out_specs = (P(None, "param", None), P())
    n = mesh.shape["param"]
    pair = mesh.shape["sensor"] == 2 and n == 16

    def body(data, spectra):
        vectors, local, _ = data.shape
        sensors, points = spectra.shape[1:3]
        fits = local % 8 == 0 and sensors == 2 * LANES and vectors % (2 * CHUNKS) == 0
        fits = fits and vectors % 8 == 0 and points * 2 * vectors == LANES
        return (paired_body if pair and fits else general_body)(data, spectra)

    return jax.shard_map(body, mesh=mesh, in_specs=in_specs, out_specs=out_specs, check_vma=False)
```

```python
import functools
import math

import jax
import jax.numpy as jnp
import numpy as np
from jax import lax
from jax.experimental import pallas as pl
from jax.experimental.pallas import tpu as pltpu
from jax.sharding import PartitionSpec as P

MESH = pl.DeviceIdType.MESH
LANES = 128
GROUP = 8
CHUNKS = 8


def spectral_tables(steps):
    length = 2 * steps
    freqs = steps + 1
    times = lax.broadcasted_iota(jnp.int32, (steps, freqs), 0)
    bins = lax.broadcasted_iota(jnp.int32, (steps, freqs), 1)
    phase = 2.0 * math.pi / length * (times * bins % length).astype(jnp.float32)
    forward = jnp.concatenate([jnp.cos(phase), -jnp.sin(phase)], axis=1)
    weight = jnp.where((bins == 0) | (bins == steps), 1.0, 2.0) / length
    backward = jnp.concatenate([(weight * jnp.cos(phase)).T, (-weight * jnp.sin(phase)).T], axis=0)
    return (forward, backward)


def to_spectrum(series, forward):
    vectors, sensors, steps = series.shape
    flat = jnp.dot(
        series.reshape(vectors * sensors, steps),
        forward,
        precision=lax.Precision.HIGHEST,
        preferred_element_type=jnp.float32,
    )
    return flat.reshape(vectors, sensors, forward.shape[1])


def contract(kernel, spectrum):
    return jnp.einsum(
        "spf,rsf->rpf",
        kernel,
        spectrum,
        precision=lax.Precision.HIGHEST,
        preferred_element_type=jnp.float32,
    )


def general_body(data, spectra):
    steps = data.shape[2]
    freqs = steps + 1
    forward, backward = spectral_tables(steps)
    whole = to_spectrum(lax.all_gather(data, "param", axis=1, tiled=True), forward)
    real_part = whole[..., :freqs]
    imag_part = whole[..., freqs:]
    kernel_re = spectra[0]
    kernel_im = spectra[1]
    out_re = contract(kernel_re, real_part) + contract(kernel_im, imag_part)
    out_im = contract(kernel_re, imag_part) - contract(kernel_im, real_part)
    vectors, points = (out_re.shape[0], out_re.shape[1])
    stacked = jnp.concatenate([out_re, out_im], axis=2).reshape(vectors * points, 2 * freqs)
    partial_field = jnp.dot(
        stacked, backward, precision=lax.Precision.HIGHEST, preferred_element_type=jnp.float32
    ).reshape(vectors, points, steps)
    count = points * lax.axis_size("param") * steps
    share = lax.psum_scatter(partial_field, "sensor", scatter_dimension=0, tiled=True)
    squares = lax.psum(jnp.sum(share * share, axis=(1, 2)), "param")
    scale = jnp.sqrt(squares / count + 1e-06)
    normalized = share / scale[:, None, None]
    gradient, rms_all = (
        lax.all_gather(normalized, "sensor", axis=0, tiled=True),
        lax.all_gather(scale, "sensor", axis=0, tiled=True),
    )
    return (gradient, rms_all)


def split(value):
    high = value.astype(jnp.bfloat16)
    return high, (value - high.astype(jnp.float32)).astype(jnp.bfloat16)


NT_DIMS = (((1,), (1,)), ((), ()))


def product(left, right, dims):
    dot = functools.partial(lax.dot_general, dimension_numbers=dims, preferred_element_type=jnp.float32)
    size = left[0].shape[0]
    both = dot(jnp.concatenate(left, axis=0), right[0])
    return both[:size] + (both[size:] + dot(left[0], right[1]))


def kernel(
    n, lines, vectors, local, steps, points, freqs, padded, wide,
    data_ref, spectra_ref, table_ref,
    out_ref, rms_ref,
    gathered, kbuf, table, even_h, even_l, odd_h, odd_l, spectrum, product_s, partial, pairs, square, squares,
    load_sem, swap_send, swap_recv, kswap_send, kswap_recv, z_send, z_recv, y_send, y_recv, c_send, c_recv,
    f_send, f_recv, r_send, r_recv,
):
    me = lax.axis_index("param")
    core = lax.axis_index("sensor")
    x = lax.rem(me, 2)
    y = lax.rem(me // 2, 2)
    z = me // 4
    plane = 4
    other_chip = me + 1 - 2 * x
    y_chip = me + 2 - 4 * y
    other_core = 1 - core
    swapped = x != core
    kept = x == core
    per = (vectors // 2) // CHUNKS

    table_copy = pltpu.make_async_copy(table_ref, table, load_sem.at[0])
    table_copy.start()
    kbuf[:, freqs:] = jnp.zeros((2, padded - freqs) + tuple(kbuf.shape[2:]), jnp.float32)

    barrier = pltpu.get_barrier_semaphore()

    @pl.loop(1, n)
    def _(step):
        pl.semaphore_signal(barrier, inc=1, device_id=(lax.rem(me + step, n), core), device_id_type=MESH)

    pl.semaphore_signal(barrier, inc=1, device_id=(me, other_core), device_id_type=MESH)
    pl.semaphore_signal(barrier, inc=1, device_id=(other_chip, other_core), device_id_type=MESH)
    pl.semaphore_wait(barrier, n + 1)

    def slot(line, row, column):
        return line * plane + row * 2 + column

    def block(chunk, position):
        return gathered.at[pl.ds(chunk * per, per), pl.ds(pl.multiple_of(position * local, local), local), :]

    mine = slot(z, y, core)

    def swap(chunk):
        return pltpu.make_async_remote_copy(
            src_ref=data_ref.at[pl.ds(chunk * per, per)],
            dst_ref=block(chunk, slot(z, y, other_core)),
            send_sem=swap_send.at[chunk], recv_sem=swap_recv.at[chunk],
            device_id=(other_chip, other_core), device_id_type=MESH,
        )

    def swap_arrival(chunk):
        return pltpu.make_async_remote_copy(
            src_ref=data_ref.at[pl.ds(chunk * per, per)], dst_ref=block(chunk, mine),
            send_sem=swap_send.at[chunk], recv_sem=swap_recv.at[chunk],
            device_id=(other_chip, other_core), device_id_type=MESH,
        )

    def keep(chunk):
        return pltpu.make_async_copy(data_ref.at[pl.ds(chunk * per, per)], block(chunk, mine), swap_recv.at[chunk])

    def kswap(part):
        return pltpu.make_async_remote_copy(
            src_ref=spectra_ref.at[part], dst_ref=kbuf.at[part, pl.ds(0, freqs)],
            send_sem=kswap_send.at[part], recv_sem=kswap_recv.at[part],
            device_id=(other_chip, other_core), device_id_type=MESH,
        )

    def kkeep(part):
        return pltpu.make_async_copy(spectra_ref.at[part], kbuf.at[part, pl.ds(0, freqs)], kswap_recv.at[part])

    @pl.when(swapped)
    def _():
        for chunk in range(CHUNKS):
            swap(chunk).start()
        for part in range(2):
            kswap(part).start()

    @pl.when(kept)
    def _():
        for chunk in range(CHUNKS):
            keep(chunk).start()
        for part in range(2):
            kkeep(part).start()

    def send(chunk, position, target, send_sem, recv_sem):
        return pltpu.make_async_remote_copy(
            src_ref=block(chunk, position), dst_ref=block(chunk, position),
            send_sem=send_sem, recv_sem=recv_sem, device_id=target, device_id_type=MESH,
        )

    def line_copy(chunk, step, way):
        source = jnp.clip(z - way * step, 0, lines - 1)
        target = jnp.clip(z + way, 0, lines - 1)
        index = step if way > 0 else lines + step
        return send(
            chunk, slot(source, y, core), (slot(target, y, x), core), z_send.at[chunk, index], z_recv.at[chunk, index]
        )

    def line_arrival(chunk, step, way):
        source = jnp.clip(z - way * (step + 1), 0, lines - 1)
        target = jnp.clip(z + way, 0, lines - 1)
        index = step if way > 0 else lines + step
        return source, send(
            chunk, slot(source, y, core), (slot(target, y, x), core), z_send.at[chunk, index], z_recv.at[chunk, index]
        )

    def sends(step, way):
        inside = z + 1 < lines if way > 0 else z > 0
        begun = z >= step if way > 0 else z + step < lines
        return jnp.logical_and(inside, begun)

    def receives(step, way):
        return z >= step + 1 if way > 0 else z + step + 1 < lines

    def y_copy(chunk, line):
        return send(chunk, slot(line, y, core), (y_chip, core), y_send.at[chunk, line], y_recv.at[chunk, line])

    def y_arrival(chunk, line):
        return send(chunk, slot(line, 1 - y, core), (y_chip, core), y_send.at[chunk, line], y_recv.at[chunk, line])

    def core_copy(chunk, row, line):
        index = row * lines + line
        return send(chunk, slot(line, row, core), (me, other_core), c_send.at[chunk, index], c_recv.at[chunk, index])

    def core_arrival(chunk, row, line):
        index = row * lines + line
        return send(
            chunk, slot(line, row, other_core), (me, other_core), c_send.at[chunk, index], c_recv.at[chunk, index]
        )

    def start_lines(chunk):
        @pl.when(swapped)
        def _():
            swap_arrival(chunk).wait_recv()

        @pl.when(kept)
        def _():
            keep(chunk).wait()

        for way in (1, -1):

            @pl.when(sends(0, way))
            def _():
                line_copy(chunk, 0, way).start()

        y_copy(chunk, z).start()
        core_copy(chunk, y, z).start()

    def from_lines(chunk):
        for step in range(lines - 1):
            for way in (1, -1):

                @pl.when(receives(step, way))
                def _():
                    source, arrival = line_arrival(chunk, step, way)
                    arrival.wait_recv()
                    if step + 1 < lines - 1:

                        @pl.when(sends(step + 1, way))
                        def _():
                            line_copy(chunk, step + 1, way).start()

                    y_copy(chunk, source).start()
                    core_copy(chunk, y, source).start()

    def from_row(chunk):
        for step in range(lines):
            line = lax.rem(z + step, lines)
            y_arrival(chunk, line).wait_recv()
            core_copy(chunk, 1 - y, line).start()

    def from_core(chunk):
        for line in range(lines):
            for row in range(2):
                core_arrival(chunk, row, line).wait_recv()

    def transform(chunk):
        @pl.loop(0, per)
        def _(pair):
            r2 = chunk * per + pair
            for half, high, low in ((0, even_h, even_l), (1, odd_h, odd_l)):
                begin = half * (gathered.shape[2] - wide)
                series = split(gathered[r2, :, begin : begin + wide])

                @pl.loop(0, 2)
                def _(imag):
                    rows = pl.ds(pl.multiple_of(imag * padded, 16), padded)
                    result = product((high[rows, :], low[rows, :]), series, NT_DIMS)
                    for lane in range(2):
                        spectrum[lane, pl.ds(imag * vectors + 2 * r2 + half, padded, stride=2 * vectors), :] = result[
                            :, lane * LANES : (lane + 1) * LANES
                        ]

    pl.loop(0, CHUNKS)(start_lines)

    table_copy.wait()
    shift = 2 * steps - (gathered.shape[2] - wide) - steps
    values = table[...]
    even_h[...], even_l[...] = split(values)
    odd_h[...], odd_l[...] = split(pltpu.roll(values, shift, 1))

    from_lines(0)

    @pl.loop(0, CHUNKS)
    def _(chunk):
        @pl.when(chunk + 1 < CHUNKS)
        def _():
            from_lines(chunk + 1)

        from_row(chunk)
        from_core(chunk)
        transform(chunk)

    @pl.when(swapped)
    def _():
        for part in range(2):
            kswap(part).wait_recv()

    @pl.when(kept)
    def _():
        for part in range(2):
            kkeep(part).wait()

    rows = GROUP * points
    columns = GROUP * 2 * vectors
    row_freq = lax.broadcasted_iota(jnp.int32, (2 * rows, columns), 0) // points % GROUP
    col_freq = lax.broadcasted_iota(jnp.int32, (2 * rows, columns), 1) // (2 * vectors)
    own = row_freq == col_freq
    lane = lax.broadcasted_iota(jnp.int32, (rows, LANES), 1)
    sign = jnp.where(lane % (2 * vectors) < vectors, 1.0, -1.0)
    row = lax.broadcasted_iota(jnp.int32, (rows, LANES), 0) // points

    @pl.loop(0, padded // GROUP, unroll=3)
    def _(group):
        begin = pl.multiple_of(group * columns, columns)
        right = split(
            jnp.concatenate([spectrum[0, pl.ds(begin, columns), :], spectrum[1, pl.ds(begin, columns), :]], axis=1)
        )
        left = jnp.concatenate(
            [kbuf[part, pl.ds(group * GROUP, GROUP)].reshape(rows, kbuf.shape[3]) for part in range(2)], axis=0
        )
        found = jnp.where(own, product(split(left), right, NT_DIMS), 0.0)
        width = columns
        while width > LANES:
            width //= 2
            found = found[:, :width] + found[:, width:]
        hop = LANES // 2
        while hop >= 2 * vectors:
            found = found + pltpu.roll(found, hop, 1)
            hop //= 2
        value = found[:rows] + sign * pltpu.roll(found[rows:], vectors, 1)
        freq = row + group * GROUP
        weight = jnp.where((freq == 0) | (freq == freqs - 1), 0.5 / steps, 1.0 / steps)
        product_s[pl.ds(pl.multiple_of(group * rows, rows), rows), :] = value * weight

    lanes = lax.broadcasted_iota(jnp.int32, (padded, LANES), 1) // (2 * vectors)
    merged = jnp.zeros((padded, LANES), jnp.float32)
    for point in range(points):
        merged = jnp.where(lanes == point, product_s[pl.ds(point, padded, stride=points), :], merged)
    turned = split(merged.T)
    plain = (((1,), (0,)), ((), ()))
    real = product(turned, (even_h[:padded, :], even_l[:padded, :]), plain)
    imag = product(turned, (even_h[padded:, :], even_l[padded:, :]), plain)
    for point in range(points):
        first = point * 2 * vectors
        field = real[first : first + vectors] + imag[first + vectors : first + 2 * vectors]
        partial[point * vectors : (point + 1) * vectors, :] = field

    def field_copy(target):
        return pltpu.make_async_remote_copy(
            src_ref=partial, dst_ref=pairs.at[x], send_sem=f_send.at[target], recv_sem=f_recv.at[x],
            device_id=(me - x + core, target), device_id_type=MESH,
        )

    def field_arrival(group):
        return pltpu.make_async_remote_copy(
            src_ref=partial, dst_ref=pairs.at[group], send_sem=f_send.at[0], recv_sem=f_recv.at[group],
            device_id=(other_chip, other_core), device_id_type=MESH,
        )

    @pl.when(swapped)
    def _():
        field_copy(0).start()
        field_copy(1).start()

    @pl.when(kept)
    def _():
        field_copy(other_core).start()
        pairs[x] = partial[...]

    field_arrival(1 - x).wait_recv()

    @pl.when(swapped)
    def _():
        field_arrival(x).wait_recv()

    total = pairs[0] + pairs[1]
    energy = total * total
    folded = energy[:vectors]
    for point in range(1, points):
        folded = folded + energy[point * vectors : (point + 1) * vectors]
    summed = jnp.broadcast_to(jnp.sum(folded, axis=1, keepdims=True), (vectors, LANES))
    square[...] = summed
    squares[me] = summed

    def square_copy(step):
        return pltpu.make_async_remote_copy(
            src_ref=square, dst_ref=squares.at[me], send_sem=r_send.at[step], recv_sem=r_recv.at[step],
            device_id=(lax.rem(me + step, n), core), device_id_type=MESH,
        )

    def square_arrival(step):
        return pltpu.make_async_remote_copy(
            src_ref=square, dst_ref=squares.at[lax.rem(me + n - step, n)],
            send_sem=r_send.at[step], recv_sem=r_recv.at[step],
            device_id=(lax.rem(me + step, n), core), device_id_type=MESH,
        )

    @pl.loop(1, n)
    def _(step):
        square_copy(step).start()

    @pl.loop(0, CHUNKS)
    def _(chunk):
        for step in range(lines - 1):
            for way in (1, -1):

                @pl.when(sends(step, way))
                def _():
                    line_copy(chunk, step, way).wait_send()

        for line in range(lines):
            y_copy(chunk, line).wait_send()
            for row in range(2):
                core_copy(chunk, row, line).wait_send()

    @pl.when(swapped)
    def _():
        for chunk in range(CHUNKS):
            swap(chunk).wait_send()
        for part in range(2):
            kswap(part).wait_send()
        field_copy(0).wait_send()
        field_copy(1).wait_send()

    @pl.when(kept)
    def _():
        field_copy(other_core).wait_send()

    @pl.loop(1, n)
    def _(step):
        square_arrival(step).wait()

    energy_all = squares[0]
    for device in range(1, n):
        energy_all = energy_all + squares[device]
    scale = jnp.sqrt(energy_all / (points * n * steps) + 1e-06)
    rms_ref[...] = scale
    inverse = scale[:, :1]
    for point in range(points):
        out_ref[point] = total[point * vectors : (point + 1) * vectors, :steps] / inverse


def paired_body(data, spectra):
    n = lax.axis_size("param")
    vectors, local, steps = data.shape
    sensors, points, freqs = spectra.shape[1:]
    wide = -(-steps // LANES) * LANES
    packed = -(-2 * steps // LANES) * LANES
    padded = -(-freqs // 16) * 16
    times = np.arange(steps)[None, :]
    bins = np.arange(freqs)[:, None]
    phase = np.pi / steps * (times * bins % (2 * steps))
    host = np.zeros((2, padded, wide), np.float32)
    host[0, :freqs, :steps] = np.cos(phase)
    host[1, :freqs, :steps] = -np.sin(phase)
    table = jnp.asarray(host.reshape(2 * padded, wide))
    lines = n // 4

    halves = data.reshape(vectors // 2, 2, local, steps)
    series = jnp.concatenate([halves[:, 0], halves[:, 1]], axis=-1)
    series = jnp.pad(series, ((0, 0), (0, 0), (0, packed - 2 * steps)))
    turned = jnp.transpose(spectra, (0, 3, 2, 1))

    hbm = pl.BlockSpec(memory_space=pl.ANY)
    vmem = pl.BlockSpec(memory_space=pltpu.VMEM)
    dma = pltpu.SemaphoreType.DMA
    f32, bf16 = jnp.float32, jnp.bfloat16
    fields, scale = pl.pallas_call(
        functools.partial(kernel, n, lines, vectors, local, steps, points, freqs, padded, wide),
        out_shape=(
            jax.ShapeDtypeStruct((points, vectors, steps), f32),
            jax.ShapeDtypeStruct((vectors, LANES), f32),
        ),
        in_specs=[hbm, hbm, hbm],
        out_specs=(vmem, vmem),
        scratch_shapes=[
            pltpu.VMEM((vectors // 2, sensors, packed), f32),
            pltpu.VMEM((2, padded, points, sensors), f32),
            pltpu.VMEM((2 * padded, wide), f32),
            pltpu.VMEM((2 * padded, wide), bf16),
            pltpu.VMEM((2 * padded, wide), bf16),
            pltpu.VMEM((2 * padded, wide), bf16),
            pltpu.VMEM((2 * padded, wide), bf16),
            pltpu.VMEM((2, padded * 2 * vectors, LANES), f32),
            pltpu.VMEM((padded * points, LANES), f32),
            pltpu.VMEM((points * vectors, wide), f32),
            pltpu.VMEM((2, points * vectors, wide), f32),
            pltpu.VMEM((vectors, LANES), f32),
            pltpu.VMEM((n, vectors, LANES), f32),
            dma((1,)),
            dma((CHUNKS,)), dma((CHUNKS,)),
            dma((2,)), dma((2,)),
            dma((CHUNKS, 2 * lines)), dma((CHUNKS, 2 * lines)),
            dma((CHUNKS, lines)), dma((CHUNKS, lines)),
            dma((CHUNKS, 2 * lines)), dma((CHUNKS, 2 * lines)),
            dma((2,)), dma((2,)),
            dma((n,)), dma((n,)),
        ],
        compiler_params=pltpu.CompilerParams(
            collective_id=0, has_side_effects=True, vmem_limit_bytes=60 * 1024 * 1024
        ),
    )(series, turned, table)
    return (jnp.transpose(fields, (1, 0, 2)), scale[:, 0])


def solution(mesh):
    in_specs = (P(None, ("sensor", "param"), None), P(None, "sensor", "param", None))
    out_specs = (P(None, "param", None), P())
    n = mesh.shape["param"]
    pair = mesh.shape["sensor"] == 2 and n == 16

    def body(data, spectra):
        vectors, local, _ = data.shape
        sensors, points = spectra.shape[1:3]
        fits = local % 8 == 0 and sensors == 2 * LANES and vectors % (2 * CHUNKS) == 0
        fits = fits and vectors % 8 == 0 and points * 2 * vectors == LANES
        return (paired_body if pair and fits else general_body)(data, spectra)

    return jax.shard_map(body, mesh=mesh, in_specs=in_specs, out_specs=out_specs, check_vma=False)
```

```python
import functools
import math

import jax
import jax.numpy as jnp
import numpy as np
from jax import lax
from jax.experimental import pallas as pl
from jax.experimental.pallas import tpu as pltpu
from jax.sharding import PartitionSpec as P

MESH = pl.DeviceIdType.MESH
LANES = 128
GROUP = 8
CHUNKS = 8


def spectral_tables(steps):
    length = 2 * steps
    freqs = steps + 1
    times = lax.broadcasted_iota(jnp.int32, (steps, freqs), 0)
    bins = lax.broadcasted_iota(jnp.int32, (steps, freqs), 1)
    phase = 2.0 * math.pi / length * (times * bins % length).astype(jnp.float32)
    forward = jnp.concatenate([jnp.cos(phase), -jnp.sin(phase)], axis=1)
    weight = jnp.where((bins == 0) | (bins == steps), 1.0, 2.0) / length
    backward = jnp.concatenate([(weight * jnp.cos(phase)).T, (-weight * jnp.sin(phase)).T], axis=0)
    return (forward, backward)


def to_spectrum(series, forward):
    vectors, sensors, steps = series.shape
    flat = jnp.dot(
        series.reshape(vectors * sensors, steps),
        forward,
        precision=lax.Precision.HIGHEST,
        preferred_element_type=jnp.float32,
    )
    return flat.reshape(vectors, sensors, forward.shape[1])


def contract(kernel, spectrum):
    return jnp.einsum(
        "spf,rsf->rpf",
        kernel,
        spectrum,
        precision=lax.Precision.HIGHEST,
        preferred_element_type=jnp.float32,
    )


def general_body(data, spectra):
    steps = data.shape[2]
    freqs = steps + 1
    forward, backward = spectral_tables(steps)
    whole = to_spectrum(lax.all_gather(data, "param", axis=1, tiled=True), forward)
    real_part = whole[..., :freqs]
    imag_part = whole[..., freqs:]
    kernel_re = spectra[0]
    kernel_im = spectra[1]
    out_re = contract(kernel_re, real_part) + contract(kernel_im, imag_part)
    out_im = contract(kernel_re, imag_part) - contract(kernel_im, real_part)
    vectors, points = (out_re.shape[0], out_re.shape[1])
    stacked = jnp.concatenate([out_re, out_im], axis=2).reshape(vectors * points, 2 * freqs)
    partial_field = jnp.dot(
        stacked, backward, precision=lax.Precision.HIGHEST, preferred_element_type=jnp.float32
    ).reshape(vectors, points, steps)
    count = points * lax.axis_size("param") * steps
    share = lax.psum_scatter(partial_field, "sensor", scatter_dimension=0, tiled=True)
    squares = lax.psum(jnp.sum(share * share, axis=(1, 2)), "param")
    scale = jnp.sqrt(squares / count + 1e-06)
    normalized = share / scale[:, None, None]
    gradient, rms_all = (
        lax.all_gather(normalized, "sensor", axis=0, tiled=True),
        lax.all_gather(scale, "sensor", axis=0, tiled=True),
    )
    return (gradient, rms_all)


def split(value):
    high = value.astype(jnp.bfloat16)
    return high, (value - high.astype(jnp.float32)).astype(jnp.bfloat16)


NT_DIMS = (((1,), (1,)), ((), ()))


def product(left, right, dims):
    dot = functools.partial(lax.dot_general, dimension_numbers=dims, preferred_element_type=jnp.float32)
    size = left[0].shape[0]
    both = dot(jnp.concatenate(left, axis=0), right[0])
    return both[:size] + (both[size:] + dot(left[0], right[1]))


def kernel(
    n, lines, vectors, local, steps, points, freqs, padded, wide,
    data_ref, spectra_ref, table_ref,
    out_ref, rms_ref,
    gathered, kbuf, table, even_h, even_l, odd_h, odd_l, spectrum, product_s, partial, pairs, square, squares,
    load_sem, swap_send, swap_recv, kswap_send, kswap_recv, z_send, z_recv, y_send, y_recv, c_send, c_recv,
    f_send, f_recv, r_send, r_recv,
):
    me = lax.axis_index("param")
    core = lax.axis_index("sensor")
    x = lax.rem(me, 2)
    y = lax.rem(me // 2, 2)
    z = me // 4
    plane = 4
    other_chip = me + 1 - 2 * x
    y_chip = me + 2 - 4 * y
    other_core = 1 - core
    swapped = x != core
    kept = x == core
    per = (vectors // 2) // CHUNKS

    table_copy = pltpu.make_async_copy(table_ref, table, load_sem.at[0])
    table_copy.start()
    kbuf[:, freqs:] = jnp.zeros((2, padded - freqs) + tuple(kbuf.shape[2:]), jnp.float32)

    barrier = pltpu.get_barrier_semaphore()

    @pl.loop(1, n)
    def _(step):
        pl.semaphore_signal(barrier, inc=1, device_id=(lax.rem(me + step, n), core), device_id_type=MESH)

    pl.semaphore_signal(barrier, inc=1, device_id=(me, other_core), device_id_type=MESH)
    pl.semaphore_signal(barrier, inc=1, device_id=(other_chip, other_core), device_id_type=MESH)
    pl.semaphore_wait(barrier, n + 1)

    def slot(line, row, column):
        return line * plane + row * 2 + column

    def block(chunk, position):
        return gathered.at[pl.ds(chunk * per, per), pl.ds(pl.multiple_of(position * local, local), local), :]

    mine = slot(z, y, core)

    def swap(chunk):
        return pltpu.make_async_remote_copy(
            src_ref=data_ref.at[pl.ds(chunk * per, per)],
            dst_ref=block(chunk, slot(z, y, other_core)),
            send_sem=swap_send.at[chunk], recv_sem=swap_recv.at[chunk],
            device_id=(other_chip, other_core), device_id_type=MESH,
        )

    def swap_arrival(chunk):
        return pltpu.make_async_remote_copy(
            src_ref=data_ref.at[pl.ds(chunk * per, per)], dst_ref=block(chunk, mine),
            send_sem=swap_send.at[chunk], recv_sem=swap_recv.at[chunk],
            device_id=(other_chip, other_core), device_id_type=MESH,
        )

    def keep(chunk):
        return pltpu.make_async_copy(data_ref.at[pl.ds(chunk * per, per)], block(chunk, mine), swap_recv.at[chunk])

    def kswap(part):
        return pltpu.make_async_remote_copy(
            src_ref=spectra_ref.at[part], dst_ref=kbuf.at[part, pl.ds(0, freqs)],
            send_sem=kswap_send.at[part], recv_sem=kswap_recv.at[part],
            device_id=(other_chip, other_core), device_id_type=MESH,
        )

    def kkeep(part):
        return pltpu.make_async_copy(spectra_ref.at[part], kbuf.at[part, pl.ds(0, freqs)], kswap_recv.at[part])

    @pl.when(swapped)
    def _():
        for chunk in range(CHUNKS):
            swap(chunk).start()
        for part in range(2):
            kswap(part).start()

    @pl.when(kept)
    def _():
        for chunk in range(CHUNKS):
            keep(chunk).start()
        for part in range(2):
            kkeep(part).start()

    def send(chunk, position, target, send_sem, recv_sem):
        return pltpu.make_async_remote_copy(
            src_ref=block(chunk, position), dst_ref=block(chunk, position),
            send_sem=send_sem, recv_sem=recv_sem, device_id=target, device_id_type=MESH,
        )

    def line_copy(chunk, step, way):
        source = jnp.clip(z - way * step, 0, lines - 1)
        target = jnp.clip(z + way, 0, lines - 1)
        index = step if way > 0 else lines + step
        return send(
            chunk, slot(source, y, core), (slot(target, y, x), core), z_send.at[chunk, index], z_recv.at[chunk, index]
        )

    def line_arrival(chunk, step, way):
        source = jnp.clip(z - way * (step + 1), 0, lines - 1)
        target = jnp.clip(z + way, 0, lines - 1)
        index = step if way > 0 else lines + step
        return source, send(
            chunk, slot(source, y, core), (slot(target, y, x), core), z_send.at[chunk, index], z_recv.at[chunk, index]
        )

    def sends(step, way):
        inside = z + 1 < lines if way > 0 else z > 0
        begun = z >= step if way > 0 else z + step < lines
        return jnp.logical_and(inside, begun)

    def receives(step, way):
        return z >= step + 1 if way > 0 else z + step + 1 < lines

    def y_copy(chunk, line):
        return send(chunk, slot(line, y, core), (y_chip, core), y_send.at[chunk, line], y_recv.at[chunk, line])

    def y_arrival(chunk, line):
        return send(chunk, slot(line, 1 - y, core), (y_chip, core), y_send.at[chunk, line], y_recv.at[chunk, line])

    def core_copy(chunk, row, line):
        index = row * lines + line
        return send(chunk, slot(line, row, core), (me, other_core), c_send.at[chunk, index], c_recv.at[chunk, index])

    def core_arrival(chunk, row, line):
        index = row * lines + line
        return send(
            chunk, slot(line, row, other_core), (me, other_core), c_send.at[chunk, index], c_recv.at[chunk, index]
        )

    def start_lines(chunk):
        @pl.when(swapped)
        def _():
            swap_arrival(chunk).wait_recv()

        @pl.when(kept)
        def _():
            keep(chunk).wait()

        for way in (1, -1):

            @pl.when(sends(0, way))
            def _():
                line_copy(chunk, 0, way).start()

        y_copy(chunk, z).start()
        core_copy(chunk, y, z).start()

    def from_lines(chunk, step):
        for way in (1, -1):

            @pl.when(receives(step, way))
            def _():
                source, arrival = line_arrival(chunk, step, way)
                arrival.wait_recv()
                if step + 1 < lines - 1:

                    @pl.when(sends(step + 1, way))
                    def _():
                        line_copy(chunk, step + 1, way).start()

                y_copy(chunk, source).start()
                core_copy(chunk, y, source).start()

    def from_row(chunk):
        for step in range(lines):
            line = lax.rem(z + step, lines)
            y_arrival(chunk, line).wait_recv()
            core_copy(chunk, 1 - y, line).start()

    def from_core(chunk):
        for line in range(lines):
            for row in range(2):
                core_arrival(chunk, row, line).wait_recv()

    def transform(chunk):
        @pl.loop(0, per)
        def _(pair):
            r2 = chunk * per + pair
            for half, high, low in ((0, even_h, even_l), (1, odd_h, odd_l)):
                begin = half * (gathered.shape[2] - wide)
                series = split(gathered[r2, :, begin : begin + wide])

                @pl.loop(0, 2)
                def _(imag):
                    rows = pl.ds(pl.multiple_of(imag * padded, 16), padded)
                    result = product((high[rows, :], low[rows, :]), series, NT_DIMS)
                    for lane in range(2):
                        spectrum[lane, pl.ds(imag * vectors + 2 * r2 + half, padded, stride=2 * vectors), :] = result[
                            :, lane * LANES : (lane + 1) * LANES
                        ]

    pl.loop(0, CHUNKS)(start_lines)

    table_copy.wait()
    shift = 2 * steps - (gathered.shape[2] - wide) - steps
    values = table[...]
    even_h[...], even_l[...] = split(values)
    odd_h[...], odd_l[...] = split(pltpu.roll(values, shift, 1))

    def finish(chunk):
        from_core(chunk)
        transform(chunk)

    stages = [functools.partial(from_lines, step=step) for step in range(lines - 1)] + [from_row, finish]

    @pl.loop(0, CHUNKS + len(stages) - 1)
    def _(turn):
        for age, stage in enumerate(stages):
            chunk = turn - age

            @pl.when(jnp.logical_and(chunk >= 0, chunk < CHUNKS))
            def _():
                stage(chunk)

    @pl.when(swapped)
    def _():
        for part in range(2):
            kswap(part).wait_recv()

    @pl.when(kept)
    def _():
        for part in range(2):
            kkeep(part).wait()

    rows = GROUP * points
    columns = GROUP * 2 * vectors
    row_freq = lax.broadcasted_iota(jnp.int32, (2 * rows, columns), 0) // points % GROUP
    col_freq = lax.broadcasted_iota(jnp.int32, (2 * rows, columns), 1) // (2 * vectors)
    own = row_freq == col_freq
    lane = lax.broadcasted_iota(jnp.int32, (rows, LANES), 1)
    sign = jnp.where(lane % (2 * vectors) < vectors, 1.0, -1.0)
    row = lax.broadcasted_iota(jnp.int32, (rows, LANES), 0) // points

    @pl.loop(0, padded // GROUP, unroll=3)
    def _(group):
        begin = pl.multiple_of(group * columns, columns)
        right = split(
            jnp.concatenate([spectrum[0, pl.ds(begin, columns), :], spectrum[1, pl.ds(begin, columns), :]], axis=1)
        )
        left = jnp.concatenate(
            [kbuf[part, pl.ds(group * GROUP, GROUP)].reshape(rows, kbuf.shape[3]) for part in range(2)], axis=0
        )
        found = jnp.where(own, product(split(left), right, NT_DIMS), 0.0)
        width = columns
        while width > LANES:
            width //= 2
            found = found[:, :width] + found[:, width:]
        hop = LANES // 2
        while hop >= 2 * vectors:
            found = found + pltpu.roll(found, hop, 1)
            hop //= 2
        value = found[:rows] + sign * pltpu.roll(found[rows:], vectors, 1)
        freq = row + group * GROUP
        weight = jnp.where((freq == 0) | (freq == freqs - 1), 0.5 / steps, 1.0 / steps)
        product_s[pl.ds(pl.multiple_of(group * rows, rows), rows), :] = value * weight

    lanes = lax.broadcasted_iota(jnp.int32, (padded, LANES), 1) // (2 * vectors)
    merged = jnp.zeros((padded, LANES), jnp.float32)
    for point in range(points):
        merged = jnp.where(lanes == point, product_s[pl.ds(point, padded, stride=points), :], merged)
    turned = split(merged.T)
    plain = (((1,), (0,)), ((), ()))
    real = product(turned, (even_h[:padded, :], even_l[:padded, :]), plain)
    imag = product(turned, (even_h[padded:, :], even_l[padded:, :]), plain)
    for point in range(points):
        first = point * 2 * vectors
        field = real[first : first + vectors] + imag[first + vectors : first + 2 * vectors]
        partial[point * vectors : (point + 1) * vectors, :] = field

    def field_copy(target):
        return pltpu.make_async_remote_copy(
            src_ref=partial, dst_ref=pairs.at[x], send_sem=f_send.at[target], recv_sem=f_recv.at[x],
            device_id=(me - x + core, target), device_id_type=MESH,
        )

    def field_arrival(group):
        return pltpu.make_async_remote_copy(
            src_ref=partial, dst_ref=pairs.at[group], send_sem=f_send.at[0], recv_sem=f_recv.at[group],
            device_id=(other_chip, other_core), device_id_type=MESH,
        )

    @pl.when(swapped)
    def _():
        field_copy(0).start()
        field_copy(1).start()

    @pl.when(kept)
    def _():
        field_copy(other_core).start()
        pairs[x] = partial[...]

    field_arrival(1 - x).wait_recv()

    @pl.when(swapped)
    def _():
        field_arrival(x).wait_recv()

    total = pairs[0] + pairs[1]
    energy = total * total
    folded = energy[:vectors]
    for point in range(1, points):
        folded = folded + energy[point * vectors : (point + 1) * vectors]
    summed = jnp.broadcast_to(jnp.sum(folded, axis=1, keepdims=True), (vectors, LANES))
    square[...] = summed
    squares[me] = summed

    def square_copy(step):
        return pltpu.make_async_remote_copy(
            src_ref=square, dst_ref=squares.at[me], send_sem=r_send.at[step], recv_sem=r_recv.at[step],
            device_id=(lax.rem(me + step, n), core), device_id_type=MESH,
        )

    def square_arrival(step):
        return pltpu.make_async_remote_copy(
            src_ref=square, dst_ref=squares.at[lax.rem(me + n - step, n)],
            send_sem=r_send.at[step], recv_sem=r_recv.at[step],
            device_id=(lax.rem(me + step, n), core), device_id_type=MESH,
        )

    @pl.loop(1, n)
    def _(step):
        square_copy(step).start()

    @pl.loop(0, CHUNKS)
    def _(chunk):
        for step in range(lines - 1):
            for way in (1, -1):

                @pl.when(sends(step, way))
                def _():
                    line_copy(chunk, step, way).wait_send()

        for line in range(lines):
            y_copy(chunk, line).wait_send()
            for row in range(2):
                core_copy(chunk, row, line).wait_send()

    @pl.when(swapped)
    def _():
        for chunk in range(CHUNKS):
            swap(chunk).wait_send()
        for part in range(2):
            kswap(part).wait_send()
        field_copy(0).wait_send()
        field_copy(1).wait_send()

    @pl.when(kept)
    def _():
        field_copy(other_core).wait_send()

    @pl.loop(1, n)
    def _(step):
        square_arrival(step).wait()

    energy_all = squares[0]
    for device in range(1, n):
        energy_all = energy_all + squares[device]
    scale = jnp.sqrt(energy_all / (points * n * steps) + 1e-06)
    rms_ref[...] = scale
    inverse = scale[:, :1]
    for point in range(points):
        out_ref[point] = total[point * vectors : (point + 1) * vectors, :steps] / inverse


def paired_body(data, spectra):
    n = lax.axis_size("param")
    vectors, local, steps = data.shape
    sensors, points, freqs = spectra.shape[1:]
    wide = -(-steps // LANES) * LANES
    packed = -(-2 * steps // LANES) * LANES
    padded = -(-freqs // 16) * 16
    times = np.arange(steps)[None, :]
    bins = np.arange(freqs)[:, None]
    phase = np.pi / steps * (times * bins % (2 * steps))
    host = np.zeros((2, padded, wide), np.float32)
    host[0, :freqs, :steps] = np.cos(phase)
    host[1, :freqs, :steps] = -np.sin(phase)
    table = jnp.asarray(host.reshape(2 * padded, wide))
    lines = n // 4

    halves = data.reshape(vectors // 2, 2, local, steps)
    series = jnp.concatenate([halves[:, 0], halves[:, 1]], axis=-1)
    series = jnp.pad(series, ((0, 0), (0, 0), (0, packed - 2 * steps)))
    turned = jnp.transpose(spectra, (0, 3, 2, 1))

    hbm = pl.BlockSpec(memory_space=pl.ANY)
    vmem = pl.BlockSpec(memory_space=pltpu.VMEM)
    dma = pltpu.SemaphoreType.DMA
    f32, bf16 = jnp.float32, jnp.bfloat16
    fields, scale = pl.pallas_call(
        functools.partial(kernel, n, lines, vectors, local, steps, points, freqs, padded, wide),
        out_shape=(
            jax.ShapeDtypeStruct((points, vectors, steps), f32),
            jax.ShapeDtypeStruct((vectors, LANES), f32),
        ),
        in_specs=[hbm, hbm, hbm],
        out_specs=(vmem, vmem),
        scratch_shapes=[
            pltpu.VMEM((vectors // 2, sensors, packed), f32),
            pltpu.VMEM((2, padded, points, sensors), f32),
            pltpu.VMEM((2 * padded, wide), f32),
            pltpu.VMEM((2 * padded, wide), bf16),
            pltpu.VMEM((2 * padded, wide), bf16),
            pltpu.VMEM((2 * padded, wide), bf16),
            pltpu.VMEM((2 * padded, wide), bf16),
            pltpu.VMEM((2, padded * 2 * vectors, LANES), f32),
            pltpu.VMEM((padded * points, LANES), f32),
            pltpu.VMEM((points * vectors, wide), f32),
            pltpu.VMEM((2, points * vectors, wide), f32),
            pltpu.VMEM((vectors, LANES), f32),
            pltpu.VMEM((n, vectors, LANES), f32),
            dma((1,)),
            dma((CHUNKS,)), dma((CHUNKS,)),
            dma((2,)), dma((2,)),
            dma((CHUNKS, 2 * lines)), dma((CHUNKS, 2 * lines)),
            dma((CHUNKS, lines)), dma((CHUNKS, lines)),
            dma((CHUNKS, 2 * lines)), dma((CHUNKS, 2 * lines)),
            dma((2,)), dma((2,)),
            dma((n,)), dma((n,)),
        ],
        compiler_params=pltpu.CompilerParams(
            collective_id=0, has_side_effects=True, vmem_limit_bytes=60 * 1024 * 1024
        ),
    )(series, turned, table)
    return (jnp.transpose(fields, (1, 0, 2)), scale[:, 0])


def solution(mesh):
    in_specs = (P(None, ("sensor", "param"), None), P(None, "sensor", "param", None))
    out_specs = (P(None, "param", None), P())
    n = mesh.shape["param"]
    pair = mesh.shape["sensor"] == 2 and n == 16

    def body(data, spectra):
        vectors, local, _ = data.shape
        sensors, points = spectra.shape[1:3]
        fits = local % 8 == 0 and sensors == 2 * LANES and vectors % (2 * CHUNKS) == 0
        fits = fits and vectors % 8 == 0 and points * 2 * vectors == LANES
        return (paired_body if pair and fits else general_body)(data, spectra)

    return jax.shard_map(body, mesh=mesh, in_specs=in_specs, out_specs=out_specs, check_vma=False)
```
